256 devices in a mesh: depth: 2 (over z_hi), row: 8 (over y, core), col: 16 (over x, z_lo).
Axes of the slice: x: 4, y: 4, z: 8 (z_hi: 2, z_lo: 4; z = z_hi * 4 + z_lo), core: 2. Of those that a mesh axis runs over, the one named last changes fastest.
Arguments:
- q_slab: float32 [6144, 1024], P('col', ('depth', 'row')), may hold values from -6 to 6
- triangle: float32 [1024, 1024], P(None, 'depth'), as said below
- panel_q: float32 [32768, 1024], P('row', ('depth', 'col')), may hold values from -0.1875 to 0.1875
Outputs:
- slab_out: float32 [6144, 32768], P('col', 'row')
The draws below stay inside these ranges and needn't reach their ends.
Inputs may be any that keep to these rules, and one draw needn't show every extreme that they name: triangle is zero below its diagonal; its diagonal lies in 0.5 to 1.5.
All inputs are finite; a program needn't handle non-finite values.
Results may differ from the reference program's by a relative error of at most 0.000071.
Values sent between devices are 32-bit elements; how exact they have to be, the bound alone decides.
No kernel may reach another device: no remote copies, remote signals or barrier semaphores. Data moves between devices by JAX's collectives and lax.ppermute only.
A program may use at most 64 MiB of HBM per device.

```python
import math
import jax
import jax.numpy as jnp
from jax import lax

ORDER = 32768
K = 1024
SLAB = 6144


def draw_triangle(key, part):
    first, second = jax.random.split(jax.random.fold_in(key, 7))
    upper = jnp.clip(jax.random.normal(first, (K, K), jnp.float32), -4.0, 4.0)
    upper = upper / math.sqrt(K)
    diagonal = jax.random.uniform(second, (K,), jnp.float32, 0.5, 1.5)
    return jnp.triu(upper, 1) + jnp.diag(diagonal)


def block_levels(rng, shape, shards, low, largest):
    def one(dim, shards_of):
        heights = jax.random.uniform(jax.random.fold_in(jax.random.fold_in(rng, 6), dim), (shards_of,), jnp.float32, low / len(shards), largest / len(shards))
        return jnp.repeat(jnp.exp(heights), shape[dim] // shards_of).reshape((-1,) + (1,) * (len(shape) - dim - 1))

    gain = one(*shards[0])
    for cut in shards[1:]:
        gain = gain * one(*cut)
    return gain


def gaussian(key, shape, deviation, most, cuts=(), dtype=jnp.bfloat16):
    array = deviation * jax.random.normal(key, shape, jnp.float32)
    if cuts:
        array = array * block_levels(key, shape, cuts, -0.22, 0.18)
    return jnp.clip(array, -most, most).astype(dtype)


def setup_inputs(seed: int = 0) -> dict:
    seeds = jax.random.split(jax.random.key(seed), 4)
    q_slab = gaussian(seeds[0], (SLAB, K), 1.0, 6.0, ((0, 16), (1, 16)), jnp.float32)
    triangle = draw_triangle(jax.random.fold_in(seeds[3], 71), 0)
    panel_q = gaussian(seeds[2], (ORDER, K), K ** -0.5, 0.1875, ((0, 8), (1, 32)), jnp.float32)
    return {"q_slab": q_slab, "triangle": triangle, "panel_q": panel_q}


def reference(q_slab, triangle, panel_q):
    left = jnp.dot(q_slab, triangle, precision=lax.Precision.HIGHEST, preferred_element_type=jnp.float32)
    return lax.dot_general(left, panel_q, (((1,), (1,)), ((), ())), precision=lax.Precision.HIGHEST, preferred_element_type=jnp.float32)
```

```python
import jax
import jax.numpy as jnp
from jax import lax
from jax.sharding import Mesh
from jax.sharding import PartitionSpec as P


Z = ("depth", "z")
ZFIRST = 2432


def shift(value, axis, by):
    count = lax.axis_size(axis)
    return lax.ppermute(
        value, axis, [(i, (i + by) % count) for i in range(count)]
    )


def product(left, right):
    return lax.dot_general(
        left,
        right,
        (((0,), (0,)), ((), ())),
        precision=lax.Precision.HIGH,
        preferred_element_type=jnp.float32,
    )


def ordered(mine, other, axis):
    first = lax.axis_index(axis) == 0
    return jnp.stack([jnp.where(first, mine, other), jnp.where(first, other, mine)])


def over_y(value):
    parts = [value, shift(value, "y", -1), shift(value, "y", -2), shift(value, "y", 1)]
    return jnp.roll(jnp.stack(parts), lax.axis_index("y"), axis=0)


def left_of(q, triangle):
    width, rows = q.shape
    half = triangle.shape[1]
    q = ordered(q, shift(q, "depth", 1), "depth")
    q = ordered(q, shift(q, "core", 1), "core")
    q = over_y(q)
    factor = triangle.reshape(2, 4, 2, width, half)
    mine = lax.dot_general(
        jnp.transpose(factor, (1, 2, 0, 3, 4)).reshape(-1, half),
        q.reshape(-1, rows),
        (((0,), (0,)), ((), ())),
        precision=lax.Precision.HIGH,
        preferred_element_type=jnp.float32,
    )
    size = half // 8
    at = lax.axis_index("y") * 2 + lax.axis_index("core")
    part = lax.dynamic_slice_in_dim(mine, at * size, size, 0)
    part = shift(part, "depth", 1)
    part = ordered(part, shift(part, "core", 1), "core")
    other = over_y(part).reshape(half, rows)
    blocks = jnp.stack([mine, other]).reshape(2, 4, 4, half // 16, rows)
    blocks = jnp.transpose(blocks, (1, 0, 2, 3, 4)).reshape(4, 8, half // 16, rows)
    blocks = jnp.roll(blocks, -lax.axis_index("x"), axis=0)
    return jnp.roll(blocks, -lax.axis_index("z"), axis=1)


def ring4(value):
    mid = value.shape[0] // 2
    right, left = shift(value, "x", 1), shift(value, "x", -1)
    far = [shift(right[:mid], "x", 1), shift(left[mid:], "x", -1)]
    return value, right, left, jnp.concatenate(far)


def ring8(value):
    mid = value.shape[0] // 2
    right, left, found = value, value, []
    for _ in range(3):
        right, left = shift(right, Z, 1), shift(left, Z, -1)
        found += [right, left]
    far = [shift(right[:mid], Z, 1), shift(left[mid:], Z, -1)]
    return [value, *found, jnp.concatenate(far)]


XS = (0, 3, 1, 2)
ZS = (0, 7, 1, 6, 2, 5, 3, 4)


def per_device(q_slab, triangle, panel_q):
    mine = panel_q.T
    near = ring8(mine[:, :ZFIRST])
    across = ring4(mine[:, ZFIRST:])
    groups = ((0, 1, 2), (3, 4, 5, 6, 7))
    wide = [ring4(jnp.concatenate([near[i] for i in group])) for group in groups]
    deep = ring8(jnp.concatenate(across))
    left = left_of(q_slab.T, triangle)

    def first(group, which):
        return jnp.concatenate([left[XS[which], ZS[i]] for i in groups[group]])

    def second(which):
        return jnp.concatenate([left[x, ZS[which]] for x in XS])

    total_z = sum(
        product(first(g, w), wide[g][w]) for g in range(2) for w in range(4)
    )
    total_x = sum(product(second(w), deep[w]) for w in range(8))
    return jnp.concatenate([total_z, total_x], axis=1)


def solution(mesh):
    torus = Mesh(
        mesh.devices.reshape(2, 4, 2, 4, 4), ("depth", "y", "core", "x", "z")
    )
    col = ("x", "z")
    row = ("y", "core")
    in_specs = (P(col, ("depth", *row)), P(None, "depth"), P(row, ("depth", *col)))
    return jax.shard_map(
        per_device,
        mesh=torus,
        in_specs=in_specs,
        out_specs=P(col, row),
        check_vma=False,
    )
```
